32 devices in a mesh: dp: 2 (over y), tm: 4 (over z), rows: 4 (over x, core).
Axes of the slice: x: 2, y: 2, z: 4, core: 2. Of those that a mesh axis runs over, the one named last changes fastest.
Arguments:
- clips: bfloat16 [2, 8, 4, 128, 256], P('dp', 'tm', 'rows'), may hold values from -12 to 12
- weight: bfloat16 [3, 3, 3, 256, 256], replicated, may hold values from -0.078125 to 0.078125
- bias: float32 [256], replicated, may hold values from -1 to 1
- head: float32 [256], replicated, may hold values from -4 to 4
Outputs:
- grad_weight: float32 [3, 3, 3, 256, 256], replicated
- grad_bias: float32 [256], replicated
- grad_head: float32 [256], replicated
The draws below stay inside these ranges and needn't reach their ends.
All inputs are finite; a program needn't handle non-finite values.
Results may differ from the reference program's by a relative error of at most 0.0003.
Values may be sent and summed in bfloat16 or wider, within the bound.
A program may use at most 128 MiB of HBM per device.

```python
import jax
import jax.numpy as jnp
from jax import lax

C = 256
WID = 128
NT = 8
NH = 4
CLIPS = 2


def draw_clips(key, part):
    shape = (CLIPS, NT, NH, WID, C)
    frame_scale = 3.0 ** (jnp.arange(NT, dtype=jnp.float32) / max(NT - 1, 1))
    values = jnp.clip(jax.random.normal(key, shape, jnp.float32), -4.0, 4.0)
    return (values * frame_scale[None, :, None, None, None]).astype(jnp.bfloat16)


def centred(key, shape, width, most, kind=jnp.bfloat16):
    return jnp.clip(width * jax.random.normal(key, shape, jnp.float32), -most, most).astype(kind)


def setup_inputs(seed: int = 0) -> dict:
    seeds = jax.random.split(jax.random.key(seed), 5)
    return {
        "clips": draw_clips(jax.random.fold_in(seeds[4], 71), 0),
        "weight": centred(seeds[1], (3, 3, 3, C, C), (27 * C) ** -0.5, 0.078125),
        "bias": jnp.clip(jax.random.uniform(seeds[2], (C,), jnp.float32, -1.0, 1.0), -1.0, 1.0),
        "head": centred(seeds[3], (C,), 1.0, 4.0, jnp.float32),
    }


penalty_weight = 0.01


def conv_offsets(padded, weight, transpose):
    nclip, tpad, rpad, wpad, chans = padded.shape
    frames, rowsn, cols = tpad - 2, rpad - 2, wpad - 2
    total = jnp.zeros((nclip * frames * rowsn * cols, weight.shape[4]), jnp.float32)
    for a in range(3):
        for b in range(3):
            for d in range(3):
                if transpose:
                    piece = padded[:, 2 - a:2 - a + frames, 2 - b:2 - b + rowsn, 2 - d:2 - d + cols]
                    total = total + lax.dot_general(piece.reshape(-1, chans), weight[a, b, d], (((1,), (1,)), ((), ())), preferred_element_type=jnp.float32)
                else:
                    piece = padded[:, a:a + frames, b:b + rowsn, d:d + cols]
                    total = total + jnp.dot(piece.reshape(-1, chans), weight[a, b, d], preferred_element_type=jnp.float32)
    return total.reshape(nclip, frames, rowsn, cols, -1)


def correlate(padded, right):
    nclip, tpad, rpad, wpad, chans = padded.shape
    frames, rowsn, cols = tpad - 2, rpad - 2, wpad - 2
    right_rows = right.reshape(-1, right.shape[-1])
    blocks = []
    for a in range(3):
        for b in range(3):
            for d in range(3):
                piece = padded[:, a:a + frames, b:b + rowsn, d:d + cols].reshape(-1, chans)
                blocks.append(lax.dot_general(piece, right_rows, (((0,), (0,)), ((), ())), preferred_element_type=jnp.float32))
    return jnp.stack(blocks).reshape(3, 3, 3, chans, right.shape[-1])


def pad_all(field):
    return jnp.pad(field, ((0, 0), (1, 1), (1, 1), (1, 1), (0, 0)))


def reference(clips, weight, bias, head):
    clip_pad = pad_all(clips)
    pre = conv_offsets(clip_pad, weight, False) + bias
    sig = jax.nn.sigmoid(pre)
    slope = sig * (1.0 + pre * (1.0 - sig))
    curve = sig * (1.0 - sig) * (2.0 + pre * (1.0 - 2.0 * sig))
    score_grad = (head * slope).astype(jnp.bfloat16)
    input_grad = conv_offsets(pad_all(score_grad), weight, True).astype(jnp.bfloat16)
    grad_pad = pad_all(input_grad)
    back_grad = penalty_weight * conv_offsets(grad_pad, weight, False)
    pre_grad = back_grad * head * curve
    pre_grad_b = pre_grad.astype(jnp.bfloat16)
    grad_weight = penalty_weight * correlate(grad_pad, score_grad) + correlate(clip_pad, pre_grad_b)
    grad_bias = jnp.sum(pre_grad, axis=(0, 1, 2, 3))
    grad_head = jnp.sum(back_grad * slope, axis=(0, 1, 2, 3))
    return grad_weight, grad_bias, grad_head
```

```python
import functools

import jax
import jax.numpy as jnp
from jax import lax
from jax.experimental import pallas as pl
from jax.experimental.pallas import tpu as pltpu
from jax.sharding import PartitionSpec as P

penalty_weight = 0.01
MESH = pl.DeviceIdType.MESH
SUB = 8
TAPS = 3


def factor_groups(sizes):
    dp, tm, rows = sizes
    if rows % 2 == 0:
        pair, far = ("rows", 1, 2), ("rows", 2, rows // 2)
    else:
        pair, far = ("rows", 1, 1), ("rows", 1, rows)
    return pair, far, ("dp", 1, dp), ("tm", 1, tm)


def make_plan(sizes, blocks):
    pair, far, depth, line = factor_groups(sizes)
    orders = [(far, depth, line), (depth, far, line)]
    unit = far[2] * depth[2] * line[2]
    half = -(-blocks // pair[2])
    units = -(-half // unit)
    parts = [(units + k) // len(orders) * unit for k in range(len(orders))]
    return pair, orders, parts, sum(parts) * pair[2]


def kernel(
    sizes, plan, clips_ref, weight_ref, bias_ref, head_ref,
    out_ref, small_ref,
    w_ref, clip_pad, score_pad, grad_pad, acc, slope_ref, curve_ref, cat_s, cat_p, total,
    full, land, small_mine, small_land,
    local_sem, halo_send, halo_recv, part_send, part_recv, gath_send, gath_recv,
    small_send, small_recv,
):
    dp, tm, rows = sizes
    frames, cols, chans = clips_ref.shape
    count = frames * cols
    me = {"dp": lax.axis_index("dp"), "tm": lax.axis_index("tm"), "rows": lax.axis_index("rows")}

    def device(**moved):
        place = dict(me, **moved)
        return (place["dp"], place["tm"], place["rows"])

    weight_copy = pltpu.make_async_copy(weight_ref, w_ref, local_sem.at[0])
    weight_copy.start()
    clip_copy = pltpu.make_async_copy(
        clips_ref, clip_pad.at[pl.ds(1, frames), 1], local_sem.at[1]
    )
    clip_copy.start()
    for pad in (clip_pad, score_pad, grad_pad):
        pad[:, 0] = jnp.zeros((frames + 2, cols, chans), pad.dtype)
        pad[:, 2] = jnp.zeros((frames + 2, cols, chans), pad.dtype)
        pad[0, 1] = jnp.zeros((cols, chans), pad.dtype)
        pad[frames + 1, 1] = jnp.zeros((cols, chans), pad.dtype)

    barrier = pltpu.get_barrier_semaphore()
    flat = me["tm"] * rows + me["rows"]
    plane = tm * rows

    def greet(step, carry):
        other = lax.rem(flat + step, plane)
        pl.semaphore_signal(
            barrier, inc=1, device_id=device(tm=other // rows, rows=lax.rem(other, rows)),
            device_id_type=MESH,
        )
        return carry

    lax.fori_loop(1, plane, greet, 0)
    for step in range(1, dp):
        pl.semaphore_signal(
            barrier, inc=1, device_id=device(dp=lax.rem(me["dp"] + step, dp)), device_id_type=MESH
        )
    pl.semaphore_wait(barrier, plane - 1 + dp - 1)

    moves = [(t, r) for t in (-1, 0, 1) for r in (-1, 0, 1) if (t, r) != (0, 0)]

    def inside(t, r):
        ok = None
        for axis, step, size in (("tm", t, tm), ("rows", r, rows)):
            if step:
                cond = me[axis] > 0 if step < 0 else me[axis] < size - 1
                ok = cond if ok is None else jnp.logical_and(ok, cond)
        return ok

    def halo_copy(which, pad, source, t, r):
        slot = which * len(moves) + moves.index((t, r))
        if t == 0:
            here, there = pl.ds(0, frames), pl.ds(1, frames)
        elif t > 0:
            here, there = pl.ds(frames - 1, 1), pl.ds(0, 1)
        else:
            here, there = pl.ds(0, 1), pl.ds(frames + 1, 1)
        return pltpu.make_async_remote_copy(
            src_ref=source.at[here], dst_ref=pad.at[there, 1 - r],
            send_sem=halo_send.at[slot], recv_sem=halo_recv.at[slot],
            device_id=device(tm=me["tm"] + t, rows=me["rows"] + r), device_id_type=MESH,
        )

    def halo_start(which, pad, source):
        for t, r in moves:
            @pl.when(inside(t, r))
            def _():
                halo_copy(which, pad, source, t, r).start()

    def halo_wait(which, pad, source):
        for t, r in moves:
            @pl.when(inside(t, r))
            def _():
                halo_copy(which, pad, source, t, r).wait_send()

            @pl.when(inside(-t, -r))
            def _():
                halo_copy(which, pad, source, t, r).wait_recv()

    column = lax.rem(lax.broadcasted_iota(jnp.int32, (count, chans), 0), cols)

    def earlier(value):
        return jnp.where(column == 0, 0.0, pltpu.roll(value, 1, 0))

    def later(value):
        return jnp.where(column == cols - 1, 0.0, pltpu.roll(value, count - 1, 0))

    def conv(pad, transpose):
        def step(a, carry):
            base = (TAPS - 1 - a) if transpose else a
            pieces = [
                pad[pl.ds(base, frames), (TAPS - 1 - b) if transpose else b].reshape(count, chans)
                for b in range(TAPS)
            ]
            left = jnp.concatenate(pieces, axis=1)
            for d in range(TAPS):
                taps = [w_ref[(a * TAPS + b) * TAPS + d] for b in range(TAPS)]
                if transpose:
                    part = lax.dot_general(
                        left, jnp.concatenate(taps, axis=1), (((1,), (1,)), ((), ())),
                        preferred_element_type=jnp.float32,
                    )
                else:
                    part = jnp.dot(
                        left, jnp.concatenate(taps, axis=0), preferred_element_type=jnp.float32
                    )
                acc[d] += part
            return carry

        acc[...] = jnp.zeros_like(acc)
        lax.fori_loop(0, TAPS, step, 0)
        if transpose:
            return later(acc[0]) + acc[1] + earlier(acc[2])
        return earlier(acc[0]) + acc[1] + later(acc[2])

    def shifted(value):
        value = value.astype(jnp.float32)
        return jnp.concatenate(
            [later(value), value, earlier(value)], axis=1
        ).astype(jnp.bfloat16)

    halo_start(0, clip_pad, clips_ref)
    clip_copy.wait()
    weight_copy.wait()
    halo_wait(0, clip_pad, clips_ref)
    pre = conv(clip_pad, False) + bias_ref[...]
    sig = jax.nn.sigmoid(pre)
    slope = sig * (1.0 + pre * (1.0 - sig))
    slope_ref[...] = slope
    curve_ref[...] = sig * (1.0 - sig) * (2.0 + pre * (1.0 - 2.0 * sig))
    score = (head_ref[...] * slope).astype(jnp.bfloat16)
    score_pad[pl.ds(1, frames), 1] = score.reshape(frames, cols, chans)
    score_own = score_pad.at[pl.ds(1, frames), 1]
    cat_s[...] = shifted(score)
    halo_start(1, score_pad, score_own)
    halo_wait(1, score_pad, score_own)

    input_grad = conv(score_pad, True).astype(jnp.bfloat16)
    grad_pad[pl.ds(1, frames), 1] = input_grad.reshape(frames, cols, chans)
    grad_own = grad_pad.at[pl.ds(1, frames), 1]
    halo_start(2, grad_pad, grad_own)
    halo_wait(2, grad_pad, grad_own)

    back = penalty_weight * conv(grad_pad, False)
    pre_grad = back * head_ref[...] * curve_ref[...]
    cat_p[...] = shifted(pre_grad.astype(jnp.bfloat16))
    small_mine[...] = jnp.zeros_like(small_mine)
    small_mine[pl.ds(0, 1)] = jnp.sum(pre_grad, axis=0, keepdims=True)
    small_mine[pl.ds(1, 1)] = jnp.sum(back * slope_ref[...], axis=0, keepdims=True)

    pair, orders, parts, padded = plan
    rows_per_tap = chans // SUB

    def correlate(ab, carry):
        a, b = ab // TAPS, lax.rem(ab, TAPS)
        dims = (((0,), (0,)), ((), ()))
        first = lax.dot_general(
            grad_pad[pl.ds(a, frames), b].reshape(count, chans), cat_s[...], dims,
            preferred_element_type=jnp.float32,
        )
        second = lax.dot_general(
            clip_pad[pl.ds(a, frames), b].reshape(count, chans), cat_p[...], dims,
            preferred_element_type=jnp.float32,
        )
        both = penalty_weight * first + second
        for d in range(TAPS):
            total[pl.ds((ab * TAPS + d) * rows_per_tap, rows_per_tap)] = both[
                :, d * chans : (d + 1) * chans
            ].reshape(rows_per_tap, SUB, chans)
        return carry

    lax.fori_loop(0, TAPS * TAPS, correlate, 0)
    used = TAPS**3 * rows_per_tap
    if padded > used:
        total[pl.ds(used, padded - used)] = jnp.zeros((padded - used, SUB, chans), jnp.float32)

    sems = {"part": 0, "gath": 0, "land": 0}

    def place_in(group):
        axis, stride, size = group
        return lax.rem(me[axis] // stride, size)

    def peer(group, step):
        axis, stride, size = group
        mine = place_in(group)
        other = lax.rem(mine + step, size)
        return other, device(**{axis: me[axis] + (other - mine) * stride})

    def scatter_start(group, base, size):
        share = size // group[2]
        copies = []
        for step in range(1, group[2]):
            other, target = peer(group, step)
            copy = pltpu.make_async_remote_copy(
                src_ref=total.at[pl.ds(base + other * share, share)],
                dst_ref=land.at[pl.ds(sems["land"], share)],
                send_sem=part_send.at[sems["part"]], recv_sem=part_recv.at[sems["part"]],
                device_id=target, device_id_type=MESH,
            )
            copy.start()
            copies.append((copy, sems["land"]))
            sems["land"] += share
            sems["part"] += 1
        return copies, base + place_in(group) * share, share

    def scatter_end(copies, base, share, dest):
        for copy, at in copies:
            copy.wait()
        if not copies and dest is total:
            return
        chunk = min(share, 9)
        while share % chunk:
            chunk -= 1

        def add(step, carry):
            here = pl.ds(base + step * chunk, chunk)
            value = total[here]
            for _, at in copies:
                value = value + land[pl.ds(at + step * chunk, chunk)]
            dest[here] = value
            return carry

        lax.fori_loop(0, share // chunk, add, 0)

    def gather_start(group, base, size):
        copies = []
        for step in range(1, group[2]):
            _, target = peer(group, step)
            block = full.at[pl.ds(base, size)]
            copy = pltpu.make_async_remote_copy(
                src_ref=block, dst_ref=block,
                send_sem=gath_send.at[sems["gath"]], recv_sem=gath_recv.at[sems["gath"]],
                device_id=target, device_id_type=MESH,
            )
            copy.start()
            copies.append(copy)
            sems["gath"] += 1
        return copies

    at = 0
    for number, group in enumerate((pair,) + orders[0]):
        copies = []
        for step in range(1, group[2]):
            _, target = peer(group, step)
            copy = pltpu.make_async_remote_copy(
                src_ref=small_mine.at[pl.ds(number * SUB, SUB)],
                dst_ref=small_land.at[pl.ds(at * SUB, SUB)],
                send_sem=small_send.at[at], recv_sem=small_recv.at[at],
                device_id=target, device_id_type=MESH,
            )
            copy.start()
            copies.append((copy, at))
            at += 1
        if number == 0:
            copies_half, half_base, half_size = scatter_start(pair, 0, padded)
            value = small_mine[pl.ds(0, SUB)]
        for copy, _ in copies:
            copy.wait()
        for _, slot in copies:
            value = value + small_land[pl.ds(slot * SUB, SUB)]
        small_mine[pl.ds((number + 1) * SUB, SUB)] = value
    small_ref[...] = value

    scatter_end(copies_half, half_base, half_size, total)
    state = [(half_base + sum(parts[:index]), size) for index, size in enumerate(parts)]
    trail = [[] for _ in orders]
    depth = len(orders[0])
    for level in range(depth):
        started = []
        for index, order in enumerate(orders):
            base, size = state[index]
            trail[index].append((base, size))
            started.append(scatter_start(order[level], base, size))
        for index in range(len(orders)):
            copies, base, share = started[index]
            scatter_end(copies, base, share, full if level == depth - 1 else total)
            state[index] = (base, share)
    for level in reversed(range(depth)):
        started = [
            gather_start(order[level], *state[index]) for index, order in enumerate(orders)
        ]
        for index in range(len(orders)):
            for copy in started[index]:
                copy.wait()
            state[index] = trail[index][level]
    last = []
    for index in range(len(orders)):
        last.extend(gather_start(pair, *state[index]))
    own = pltpu.make_async_copy(
        full.at[pl.ds(half_base, half_size)], out_ref.at[pl.ds(half_base, half_size)],
        local_sem.at[2],
    )
    own.start()
    for copy in last:
        copy.wait()
    own.wait()
    if pair[2] > 1:
        other_base = (1 - place_in(pair)) * half_size
        rest = pltpu.make_async_copy(
            full.at[pl.ds(other_base, half_size)], out_ref.at[pl.ds(other_base, half_size)],
            local_sem.at[3],
        )
        rest.start()
        rest.wait()


def per_device(sizes, clips, weight, bias, head):
    _, frames, _, cols, chans = clips.shape
    count = frames * cols
    used = TAPS**3 * chans // SUB
    plan = make_plan(sizes, used)
    pair, orders, parts, padded = plan
    land = padded // pair[2] * (pair[2] - 1)
    parts_n, small_n = pair[2] - 1, sum(g[2] - 1 for g in (pair,) + orders[0])
    gath_n = (pair[2] - 1) * len(orders)
    for order, size in zip(orders, parts):
        for group in order:
            land += size // group[2] * (group[2] - 1)
            parts_n += group[2] - 1
            gath_n += group[2] - 1
            size //= group[2]
    pad = pltpu.VMEM((frames + 2, 3, cols, chans), jnp.bfloat16)
    field = pltpu.VMEM((count, chans), jnp.float32)
    dma = pltpu.SemaphoreType.DMA
    vmem = pl.BlockSpec(memory_space=pltpu.VMEM)
    hbm = pl.BlockSpec(memory_space=pl.ANY)
    grad_weight, small = pl.pallas_call(
        functools.partial(kernel, sizes, plan),
        out_shape=(
            jax.ShapeDtypeStruct((padded, SUB, chans), jnp.float32),
            jax.ShapeDtypeStruct((SUB, chans), jnp.float32),
        ),
        in_specs=[hbm, hbm, vmem, vmem],
        out_specs=(hbm, vmem),
        scratch_shapes=[
            pltpu.VMEM((TAPS**3, chans, chans), jnp.bfloat16),
            pad, pad, pad,
            pltpu.VMEM((TAPS, count, chans), jnp.float32),
            field, field,
            pltpu.VMEM((count, TAPS * chans), jnp.bfloat16),
            pltpu.VMEM((count, TAPS * chans), jnp.bfloat16),
            pltpu.VMEM((padded, SUB, chans), jnp.float32),
            pltpu.VMEM((padded, SUB, chans), jnp.float32),
            pltpu.VMEM((land, SUB, chans), jnp.float32),
            pltpu.VMEM((5 * SUB, chans), jnp.float32),
            pltpu.VMEM((max(small_n, 1) * SUB, chans), jnp.float32),
            dma((4,)), dma((24,)), dma((24,)),
            dma((max(parts_n, 1),)), dma((max(parts_n, 1),)),
            dma((max(gath_n, 1),)), dma((max(gath_n, 1),)),
            dma((max(small_n, 1),)), dma((max(small_n, 1),)),
        ],
        compiler_params=pltpu.CompilerParams(
            collective_id=0, has_side_effects=True, vmem_limit_bytes=60 * 1024 * 1024
        ),
    )(
        clips.reshape(frames, cols, chans),
        weight.reshape(TAPS**3, chans, chans),
        bias.reshape(1, chans),
        head.reshape(1, chans),
    )
    if padded != used:
        grad_weight = grad_weight[:used]
    return grad_weight.reshape(TAPS, TAPS, TAPS, chans, chans), small[0], small[1]


def solution(mesh):
    sizes = tuple(mesh.shape[axis] for axis in ("dp", "tm", "rows"))
    return jax.shard_map(
        functools.partial(per_device, sizes),
        mesh=mesh,
        in_specs=(P("dp", "tm", "rows", None, None), P(), P(), P()),
        out_specs=(P(), P(), P()),
        check_vma=False,
    )
```

```python
import functools
import math

import jax
import jax.numpy as jnp
from jax import lax
from jax.experimental import pallas as pl
from jax.experimental.pallas import tpu as pltpu
from jax.sharding import PartitionSpec as P

penalty_weight = 0.01
MESH = pl.DeviceIdType.MESH
SUB = 8
TAPS = 3
SPAN = 120.0


def make_plan(sizes, shares):
    dp, tm, rows = sizes
    cuts, rest, left = [], [], shares
    near = 2 if rows % 2 == 0 else 1
    for axis, stride, count in (("rows", 1, near), ("rows", near, rows // near), ("dp", 1, dp), ("tm", 1, tm)):
        cut = 1
        while count % (2 * cut) == 0 and left % (2 * cut) == 0:
            cut *= 2
        left //= cut
        cuts.append((axis, stride, cut))
        rest.append((axis, stride * cut, count // cut))
    pair, far, depth, line = cuts
    rest = tuple(group for group in rest if group[2] > 1)
    return pair, ((far, depth, line), (depth, far, line)), rest


def kernel(
    sizes, plan, clips_ref, weight_ref, bias_ref, head_ref,
    out_ref, small_ref,
    w_ref, clip_pad, score_pad, grad_pad, acc, slope_ref, curve_ref, cat_s, cat_p, total,
    land_pair, code, land, full, small_mine, small_land,
    local_sem, halo_send, halo_recv, pair_send, pair_recv, part_send, part_recv, gath_send, gath_recv,
    small_send, small_recv,
):
    dp, tm, rows = sizes
    frames, cols, chans = clips_ref.shape
    count = frames * cols
    me = {"dp": lax.axis_index("dp"), "tm": lax.axis_index("tm"), "rows": lax.axis_index("rows")}

    def device(**moved):
        place = dict(me, **moved)
        return (place["dp"], place["tm"], place["rows"])

    weight_copy = pltpu.make_async_copy(weight_ref, w_ref, local_sem.at[0])
    weight_copy.start()
    clip_copy = pltpu.make_async_copy(
        clips_ref, clip_pad.at[pl.ds(1, frames), 1], local_sem.at[1]
    )
    clip_copy.start()
    for pad in (clip_pad, score_pad, grad_pad):
        pad[:, 0] = jnp.zeros((frames + 2, cols, chans), pad.dtype)
        pad[:, 2] = jnp.zeros((frames + 2, cols, chans), pad.dtype)
        pad[0, 1] = jnp.zeros((cols, chans), pad.dtype)
        pad[frames + 1, 1] = jnp.zeros((cols, chans), pad.dtype)

    barrier = pltpu.get_barrier_semaphore()
    flat = me["tm"] * rows + me["rows"]
    plane = tm * rows

    def greet(step, carry):
        other = lax.rem(flat + step, plane)
        pl.semaphore_signal(
            barrier, inc=1, device_id=device(tm=other // rows, rows=lax.rem(other, rows)),
            device_id_type=MESH,
        )
        return carry

    lax.fori_loop(1, plane, greet, 0)
    for step in range(1, dp):
        pl.semaphore_signal(
            barrier, inc=1, device_id=device(dp=lax.rem(me["dp"] + step, dp)), device_id_type=MESH
        )
    pl.semaphore_wait(barrier, plane - 1 + dp - 1)

    moves = [(t, r) for t in (-1, 0, 1) for r in (-1, 0, 1) if (t, r) != (0, 0)]

    def inside(t, r):
        ok = None
        for axis, step, size in (("tm", t, tm), ("rows", r, rows)):
            if step:
                cond = me[axis] > 0 if step < 0 else me[axis] < size - 1
                ok = cond if ok is None else jnp.logical_and(ok, cond)
        return ok

    def halo_copy(which, pad, source, t, r):
        slot = which * len(moves) + moves.index((t, r))
        if t == 0:
            here, there = pl.ds(0, frames), pl.ds(1, frames)
        elif t > 0:
            here, there = pl.ds(frames - 1, 1), pl.ds(0, 1)
        else:
            here, there = pl.ds(0, 1), pl.ds(frames + 1, 1)
        return pltpu.make_async_remote_copy(
            src_ref=source.at[here], dst_ref=pad.at[there, 1 - r],
            send_sem=halo_send.at[slot], recv_sem=halo_recv.at[slot],
            device_id=device(tm=me["tm"] + t, rows=me["rows"] + r), device_id_type=MESH,
        )

    def halo_start(which, pad, source):
        for t, r in moves:
            @pl.when(inside(t, r))
            def _():
                halo_copy(which, pad, source, t, r).start()

    def halo_wait(which, pad, source):
        for t, r in moves:
            @pl.when(inside(t, r))
            def _():
                halo_copy(which, pad, source, t, r).wait_send()

            @pl.when(inside(-t, -r))
            def _():
                halo_copy(which, pad, source, t, r).wait_recv()

    column = lax.rem(lax.broadcasted_iota(jnp.int32, (count, chans), 0), cols)

    def earlier(value):
        return jnp.where(column == 0, 0.0, pltpu.roll(value, 1, 0))

    def later(value):
        return jnp.where(column == cols - 1, 0.0, pltpu.roll(value, count - 1, 0))

    def conv(pad, transpose):
        def step(a, carry):
            base = (TAPS - 1 - a) if transpose else a
            pieces = [
                pad[pl.ds(base, frames), (TAPS - 1 - b) if transpose else b].reshape(count, chans)
                for b in range(TAPS)
            ]
            left = jnp.concatenate(pieces, axis=1)
            for d in range(TAPS):
                taps = [w_ref[(a * TAPS + b) * TAPS + d] for b in range(TAPS)]
                if transpose:
                    part = lax.dot_general(
                        left, jnp.concatenate(taps, axis=1), (((1,), (1,)), ((), ())),
                        preferred_element_type=jnp.float32,
                    )
                else:
                    part = jnp.dot(
                        left, jnp.concatenate(taps, axis=0), preferred_element_type=jnp.float32
                    )
                acc[d] += part
            return carry

        acc[...] = jnp.zeros_like(acc)
        lax.fori_loop(0, TAPS, step, 0)
        if transpose:
            return later(acc[0]) + acc[1] + earlier(acc[2])
        return earlier(acc[0]) + acc[1] + later(acc[2])

    def shifted(value):
        value = value.astype(jnp.float32)
        return jnp.concatenate(
            [later(value), value, earlier(value)], axis=1
        ).astype(jnp.bfloat16)

    halo_start(0, clip_pad, clips_ref)
    clip_copy.wait()
    weight_copy.wait()
    halo_wait(0, clip_pad, clips_ref)
    pre = conv(clip_pad, False) + bias_ref[...]
    sig = jax.nn.sigmoid(pre)
    slope = sig * (1.0 + pre * (1.0 - sig))
    slope_ref[...] = slope
    curve_ref[...] = sig * (1.0 - sig) * (2.0 + pre * (1.0 - 2.0 * sig))
    score = (head_ref[...] * slope).astype(jnp.bfloat16)
    score_pad[pl.ds(1, frames), 1] = score.reshape(frames, cols, chans)
    score_own = score_pad.at[pl.ds(1, frames), 1]
    cat_s[...] = shifted(score)
    halo_start(1, score_pad, score_own)
    halo_wait(1, score_pad, score_own)

    input_grad = conv(score_pad, True).astype(jnp.bfloat16)
    grad_pad[pl.ds(1, frames), 1] = input_grad.reshape(frames, cols, chans)
    grad_own = grad_pad.at[pl.ds(1, frames), 1]
    halo_start(2, grad_pad, grad_own)
    halo_wait(2, grad_pad, grad_own)

    back = penalty_weight * conv(grad_pad, False)
    pre_grad = back * head_ref[...] * curve_ref[...]
    cat_p[...] = shifted(pre_grad.astype(jnp.bfloat16))
    small_mine[...] = jnp.zeros_like(small_mine)
    small_mine[pl.ds(0, 1)] = jnp.sum(pre_grad, axis=0, keepdims=True)
    small_mine[pl.ds(1, 1)] = jnp.sum(back * slope_ref[...], axis=0, keepdims=True)

    pair, orders, rest = plan
    parts, shares, taps = total.shape[:3]
    lanes = chans // parts
    half = shares // pair[2]
    units = chans // SUB

    def place_in(group):
        axis, stride, size = group
        return lax.rem(me[axis] // stride, size)

    def peer(group, step):
        axis, stride, size = group
        mine = place_in(group)
        other = lax.rem(mine + step, size)
        return other, device(**{axis: me[axis] + (other - mine) * stride})

    def pair_copy(ab):
        other, target = peer(pair, 1)
        here = pl.ds(ab * TAPS, TAPS)
        return pltpu.make_async_remote_copy(
            src_ref=total.at[:, pl.ds(other * half, half), here], dst_ref=land_pair.at[:, :, here],
            send_sem=pair_send.at[ab], recv_sem=pair_recv.at[ab],
            device_id=target, device_id_type=MESH,
        )

    def correlate(ab, carry):
        a, b = ab // TAPS, lax.rem(ab, TAPS)
        dims = (((0,), (0,)), ((), ()))
        first = lax.dot_general(
            grad_pad[pl.ds(a, frames), b].reshape(count, chans), cat_s[...], dims,
            preferred_element_type=jnp.float32,
        )
        second = lax.dot_general(
            clip_pad[pl.ds(a, frames), b].reshape(count, chans), cat_p[...], dims,
            preferred_element_type=jnp.float32,
        )
        both = penalty_weight * first + second
        for d in range(TAPS):
            for p in range(parts):
                at = d * chans + p * lanes
                total[p, :, ab * TAPS + d] = both[:, at : at + lanes].reshape(units, SUB, lanes)
        if pair[2] > 1:
            @pl.when(ab > 0)
            def _():
                pair_copy(ab - 1).start()
        return carry

    lax.fori_loop(0, TAPS * TAPS, correlate, 0)

    def finish_pair():
        if pair[2] == 1:
            return
        pair_copy(TAPS * TAPS - 1).start()
        mine = place_in(pair) * half

        def wait(ab, carry):
            pair_copy(ab).wait()
            return carry

        lax.fori_loop(0, TAPS * TAPS, wait, 0)

        def add(step, carry):
            for p in range(parts):
                total[p, mine + step] = total[p, mine + step] + land_pair[p, step]
            return carry

        lax.fori_loop(0, half, add, 0)

    def encode(value):
        top = (jnp.max(jnp.abs(value), axis=0) * 1.01 + 1e-30).astype(jnp.bfloat16)
        rate = SPAN / top.astype(jnp.float32)
        return jnp.exp2(value * rate[None]).astype(jnp.bfloat16), top

    sems = {"part": 0, "gath": 0, "land": 0}

    def scatter_start(p, group, base, size, whole=False):
        share = size if whole else size // group[2]
        copies = []
        for step in range(1, group[2]):
            other, target = peer(group, step)
            origin = base if whole else base + other * share
            at = sems["land"]

            def fill(k, carry):
                value, top = encode(total[p, origin + k])
                code[at + k, pl.ds(0, taps)] = value
                code[at + k, taps] = top
                return carry

            lax.fori_loop(0, share, fill, 0)
            copy = pltpu.make_async_remote_copy(
                src_ref=code.at[pl.ds(at, share)], dst_ref=land.at[pl.ds(at, share)],
                send_sem=part_send.at[sems["part"]], recv_sem=part_recv.at[sems["part"]],
                device_id=target, device_id_type=MESH,
            )
            copy.start()
            copies.append((copy, at))
            sems["land"] += share
            sems["part"] += 1
        return copies, base if whole else base + place_in(group) * share, share

    def scatter_end(p, copies, base, share):
        for copy, _ in copies:
            copy.wait()
        if not copies:
            return

        def add(step, carry):
            value = total[p, base + step]
            for _, at in copies:
                value = value + decode(land[at + step], taps)
            total[p, base + step] = value
            return carry

        lax.fori_loop(0, share, add, 0)

    def gather_start(p, group, base, size):
        copies = []
        for step in range(1, group[2]):
            _, target = peer(group, step)
            block = full.at[p, pl.ds(base, size)]
            copy = pltpu.make_async_remote_copy(
                src_ref=block, dst_ref=block,
                send_sem=gath_send.at[sems["gath"]], recv_sem=gath_recv.at[sems["gath"]],
                device_id=target, device_id_type=MESH,
            )
            copy.start()
            copies.append(copy)
            sems["gath"] += 1
        return copies

    finish_pair()
    base = place_in(pair) * half
    state = [(base, half)] * parts
    trail = [[] for _ in range(parts)]
    depth = len(orders[0])

    def small_start(number, group, at):
        copies = []
        for step in range(1, group[2]):
            _, target = peer(group, step)
            copy = pltpu.make_async_remote_copy(
                src_ref=small_mine.at[pl.ds(number * SUB, SUB)],
                dst_ref=small_land.at[pl.ds(at * SUB, SUB)],
                send_sem=small_send.at[at], recv_sem=small_recv.at[at],
                device_id=target, device_id_type=MESH,
            )
            copy.start()
            copies.append((copy, at))
            at += 1
        return copies

    def small_end(number, copies):
        value = small_mine[pl.ds(number * SUB, SUB)]
        for copy, _ in copies:
            copy.wait()
        for _, slot in copies:
            value = value + small_land[pl.ds(slot * SUB, SUB)]
        small_mine[pl.ds((number + 1) * SUB, SUB)] = value

    small_groups = (pair,) + orders[0] + rest
    small_at = 0
    steps = [[order[level] for order in orders] for level in range(depth)]
    steps += [[group] * parts for group in rest]
    for level, groups in enumerate(steps):
        whole = level >= depth
        started = []
        for p, group in enumerate(groups):
            if not whole:
                trail[p].append(state[p])
            started.append(scatter_start(p, group, *state[p], whole))
        small = small_start(level, small_groups[level], small_at)
        small_at += len(small)
        for p in range(parts):
            copies, base, share = started[p]
            scatter_end(p, copies, base, share)
            state[p] = (base, share)
        small_end(level, small)
    for p in range(parts):
        base, size = state[p]

        def keep(k, carry):
            value, top = encode(total[p, base + k])
            full[p, base + k, pl.ds(0, taps)] = value
            full[p, base + k, taps] = top
            return carry

        lax.fori_loop(0, size, keep, 0)
    last_small = len(steps)
    small = small_start(last_small, small_groups[last_small], small_at)
    for level in reversed(range(depth)):
        started = [gather_start(p, orders[p][level], *state[p]) for p in range(parts)]
        for p in range(parts):
            for copy in started[p]:
                copy.wait()
            state[p] = trail[p][level]
    small_end(last_small, small)
    small_ref[...] = small_mine[pl.ds((last_small + 1) * SUB, SUB)]
    last = []
    for p in range(parts):
        last.extend(gather_start(p, pair, *state[p]))
    here = pl.ds(place_in(pair) * half, half)
    own = pltpu.make_async_copy(full.at[:, here], out_ref.at[:, here], local_sem.at[2])
    own.start()
    for copy in last:
        copy.wait()
    if pair[2] > 1:
        there = pl.ds((1 - place_in(pair)) * half, half)
        other = pltpu.make_async_copy(full.at[:, there], out_ref.at[:, there], local_sem.at[3])
        other.start()
        other.wait()
    own.wait()


def decode(block, taps):
    unit = block[taps].astype(jnp.float32) * (1.0 / (SPAN * math.log(2.0)))
    return jnp.log(block[:taps].astype(jnp.float32)) * unit[None]


def decode_kernel(code_ref, out_ref):
    parts, shares, blocks, _, lanes = code_ref.shape
    for p in range(parts):
        for k in range(shares):
            out_ref[:, k, :, p * lanes : (p + 1) * lanes] = decode(code_ref[p, k], blocks - 1)


def per_device(sizes, clips, weight, bias, head):
    _, frames, _, cols, chans = clips.shape
    count = frames * cols
    taps, shares, parts = TAPS**3, chans // SUB, 2
    lanes = chans // parts
    plan = make_plan(sizes, shares)
    pair, orders, rest = plan
    half = shares // pair[2]
    small_n = sum(g[2] - 1 for g in (pair,) + orders[0] + rest)
    land = parts_n = gath_n = 0
    for order in orders:
        size = half
        for group in order:
            land += size // group[2] * (group[2] - 1)
            size //= group[2]
            parts_n += group[2] - 1
        for group in rest:
            land += size * (group[2] - 1)
            parts_n += group[2] - 1
        gath_n += sum(g[2] - 1 for g in order) + pair[2] - 1
    pad = pltpu.VMEM((frames + 2, 3, cols, chans), jnp.bfloat16)
    field = pltpu.VMEM((count, chans), jnp.float32)
    coded = pltpu.VMEM((max(land, 1), taps + 1, SUB, lanes), jnp.bfloat16)
    dma = pltpu.SemaphoreType.DMA
    vmem = pl.BlockSpec(memory_space=pltpu.VMEM)
    hbm = pl.BlockSpec(memory_space=pl.ANY)
    code, small = pl.pallas_call(
        functools.partial(kernel, sizes, plan),
        out_shape=(
            jax.ShapeDtypeStruct((parts, shares, taps + 1, SUB, lanes), jnp.bfloat16),
            jax.ShapeDtypeStruct((SUB, chans), jnp.float32),
        ),
        in_specs=[hbm, hbm, vmem, vmem],
        out_specs=(hbm, vmem),
        scratch_shapes=[
            pltpu.VMEM((taps, chans, chans), jnp.bfloat16),
            pad, pad, pad,
            pltpu.VMEM((TAPS, count, chans), jnp.float32),
            field, field,
            pltpu.VMEM((count, TAPS * chans), jnp.bfloat16),
            pltpu.VMEM((count, TAPS * chans), jnp.bfloat16),
            pltpu.VMEM((parts, shares, taps, SUB, lanes), jnp.float32),
            pltpu.VMEM((parts, half, taps, SUB, lanes), jnp.float32),
            coded, coded,
            pltpu.VMEM((parts, shares, taps + 1, SUB, lanes), jnp.bfloat16),
            pltpu.VMEM(((len(rest) + 6) * SUB, chans), jnp.float32),
            pltpu.VMEM((max(small_n, 1) * SUB, chans), jnp.float32),
            dma((4,)), dma((24,)), dma((24,)), dma((TAPS**2,)), dma((TAPS**2,)),
            dma((max(parts_n, 1),)), dma((max(parts_n, 1),)),
            dma((max(gath_n, 1),)), dma((max(gath_n, 1),)),
            dma((max(small_n, 1),)), dma((max(small_n, 1),)),
        ],
        compiler_params=pltpu.CompilerParams(
            collective_id=0, has_side_effects=True, vmem_limit_bytes=60 * 1024 * 1024
        ),
    )(
        clips.reshape(frames, cols, chans),
        weight.reshape(taps, chans, chans),
        bias.reshape(1, chans),
        head.reshape(1, chans),
    )
    step = math.gcd(shares, 4)
    grad_weight = pl.pallas_call(
        decode_kernel,
        out_shape=jax.ShapeDtypeStruct((taps, shares, SUB, chans), jnp.float32),
        grid=(shares // step,),
        in_specs=[pl.BlockSpec((parts, step, taps + 1, SUB, lanes), lambda i: (0, i, 0, 0, 0))],
        out_specs=pl.BlockSpec((taps, step, SUB, chans), lambda i: (0, i, 0, 0)),
    )(code)
    return grad_weight.reshape(TAPS, TAPS, TAPS, chans, chans), small[0], small[1]


def solution(mesh):
    sizes = tuple(mesh.shape[axis] for axis in ("dp", "tm", "rows"))
    return jax.shard_map(
        functools.partial(per_device, sizes),
        mesh=mesh,
        in_specs=(P("dp", "tm", "rows", None, None), P(), P(), P()),
        out_specs=(P(), P(), P()),
        check_vma=False,
    )
```

```python
import functools
import math

import jax
import jax.numpy as jnp
from jax import lax
from jax.experimental import pallas as pl
from jax.experimental.pallas import tpu as pltpu
from jax.sharding import PartitionSpec as P

penalty_weight = 0.01
MESH = pl.DeviceIdType.MESH
SUB = 8
TAPS = 3
SPAN = 120.0


def make_plan(sizes, shares):
    dp, tm, rows = sizes
    cuts, rest, left = [], [], shares
    near = 2 if rows % 2 == 0 else 1
    for axis, stride, count in (("rows", 1, near), ("rows", near, rows // near), ("dp", 1, dp), ("tm", 1, tm)):
        cut = 1
        while count % (2 * cut) == 0 and left % (2 * cut) == 0:
            cut *= 2
        left //= cut
        cuts.append((axis, stride, cut))
        rest.append((axis, stride * cut, count // cut))
    pair, far, depth, line = cuts
    rest = tuple(group for group in rest if group[2] > 1)
    across, along, ahead = (far, depth, line), (depth, far, line), (line, depth, far)
    return pair, (ahead, along, across, along, across, across), rest


def kernel(
    sizes, plan, clips_ref, weight_ref, bias_ref, head_ref,
    out_ref, bias_out, head_out,
    w_ref, clip_pad, score_pad, grad_pad, acc, slope_ref, curve_ref, cat_s, cat_p, total,
    land_pair, code, land, full, small_mine, small_land,
    local_sem, halo_send, halo_recv, pair_send, pair_recv, part_send, part_recv, gath_send, gath_recv,
    small_send, small_recv, out_sem,
):
    small_refs = (bias_out, head_out)
    dp, tm, rows = sizes
    frames, cols, chans = clips_ref.shape
    count = frames * cols
    me = {"dp": lax.axis_index("dp"), "tm": lax.axis_index("tm"), "rows": lax.axis_index("rows")}

    def device(**moved):
        place = dict(me, **moved)
        return (place["dp"], place["tm"], place["rows"])

    weight_copy = pltpu.make_async_copy(weight_ref, w_ref, local_sem.at[0])
    weight_copy.start()
    clip_copy = pltpu.make_async_copy(
        clips_ref, clip_pad.at[pl.ds(1, frames), 1], local_sem.at[1]
    )
    clip_copy.start()
    for pad in (clip_pad, score_pad, grad_pad):
        pad[:, 0] = jnp.zeros((frames + 2, cols, chans), pad.dtype)
        pad[:, 2] = jnp.zeros((frames + 2, cols, chans), pad.dtype)
        pad[0, 1] = jnp.zeros((cols, chans), pad.dtype)
        pad[frames + 1, 1] = jnp.zeros((cols, chans), pad.dtype)

    barrier = pltpu.get_barrier_semaphore()
    flat = me["tm"] * rows + me["rows"]
    plane = tm * rows

    def greet(step, carry):
        other = lax.rem(flat + step, plane)
        pl.semaphore_signal(
            barrier, inc=1, device_id=device(tm=other // rows, rows=lax.rem(other, rows)),
            device_id_type=MESH,
        )
        return carry

    lax.fori_loop(1, plane, greet, 0)
    for step in range(1, dp):
        pl.semaphore_signal(
            barrier, inc=1, device_id=device(dp=lax.rem(me["dp"] + step, dp)), device_id_type=MESH
        )
    pl.semaphore_wait(barrier, plane - 1 + dp - 1)

    moves = [(t, r) for t in (-1, 0, 1) for r in (-1, 0, 1) if (t, r) != (0, 0)]

    def inside(t, r):
        ok = None
        for axis, step, size in (("tm", t, tm), ("rows", r, rows)):
            if step:
                cond = me[axis] > 0 if step < 0 else me[axis] < size - 1
                ok = cond if ok is None else jnp.logical_and(ok, cond)
        return ok

    def halo_copy(which, pad, source, t, r):
        slot = which * len(moves) + moves.index((t, r))
        if t == 0:
            here, there = pl.ds(0, frames), pl.ds(1, frames)
        elif t > 0:
            here, there = pl.ds(frames - 1, 1), pl.ds(0, 1)
        else:
            here, there = pl.ds(0, 1), pl.ds(frames + 1, 1)
        return pltpu.make_async_remote_copy(
            src_ref=source.at[here], dst_ref=pad.at[there, 1 - r],
            send_sem=halo_send.at[slot], recv_sem=halo_recv.at[slot],
            device_id=device(tm=me["tm"] + t, rows=me["rows"] + r), device_id_type=MESH,
        )

    def halo_start(which, pad, source):
        for t, r in moves:
            @pl.when(inside(t, r))
            def _():
                halo_copy(which, pad, source, t, r).start()

    def halo_wait(which, pad, source, level):
        for t, r in moves:
            if (t == 0) != level:
                continue

            @pl.when(inside(t, r))
            def _():
                halo_copy(which, pad, source, t, r).wait_send()

            @pl.when(inside(-t, -r))
            def _():
                halo_copy(which, pad, source, t, r).wait_recv()

    column = lax.rem(lax.broadcasted_iota(jnp.int32, (count, chans), 0), cols)

    def earlier(value):
        return jnp.where(column == 0, 0.0, pltpu.roll(value, 1, 0))

    def later(value):
        return jnp.where(column == cols - 1, 0.0, pltpu.roll(value, count - 1, 0))

    def conv(which, pad, source, transpose):
        def step(a):
            base = (TAPS - 1 - a) if transpose else a
            pieces = [
                pad[pl.ds(base, frames), (TAPS - 1 - b) if transpose else b].reshape(count, chans)
                for b in range(TAPS)
            ]
            left = jnp.concatenate(pieces, axis=1)
            for d in range(TAPS):
                taps = [w_ref[(a * TAPS + b) * TAPS + d] for b in range(TAPS)]
                if transpose:
                    part = lax.dot_general(
                        left, jnp.concatenate(taps, axis=1), (((1,), (1,)), ((), ())),
                        preferred_element_type=jnp.float32,
                    )
                else:
                    part = jnp.dot(
                        left, jnp.concatenate(taps, axis=0), preferred_element_type=jnp.float32
                    )
                acc[d] = part if a == 1 else acc[d] + part

        halo_wait(which, pad, source, True)
        step(1)
        halo_wait(which, pad, source, False)
        step(0)
        step(2)
        if transpose:
            return later(acc[0]) + acc[1] + earlier(acc[2])
        return earlier(acc[0]) + acc[1] + later(acc[2])

    def shifted(value):
        value = value.astype(jnp.float32)
        return jnp.concatenate(
            [later(value), value, earlier(value)], axis=1
        ).astype(jnp.bfloat16)

    halo_start(0, clip_pad, clips_ref)
    clip_copy.wait()
    weight_copy.wait()
    pre = conv(0, clip_pad, clips_ref, False) + bias_ref[...]
    sig = jax.nn.sigmoid(pre)
    slope = sig * (1.0 + pre * (1.0 - sig))
    slope_ref[...] = slope
    curve_ref[...] = sig * (1.0 - sig) * (2.0 + pre * (1.0 - 2.0 * sig))
    score = (head_ref[...] * slope).astype(jnp.bfloat16)
    score_pad[pl.ds(1, frames), 1] = score.reshape(frames, cols, chans)
    score_own = score_pad.at[pl.ds(1, frames), 1]
    cat_s[...] = shifted(score)
    halo_start(1, score_pad, score_own)

    input_grad = conv(1, score_pad, score_own, True).astype(jnp.bfloat16)
    grad_pad[pl.ds(1, frames), 1] = input_grad.reshape(frames, cols, chans)
    grad_own = grad_pad.at[pl.ds(1, frames), 1]
    halo_start(2, grad_pad, grad_own)

    back = penalty_weight * conv(2, grad_pad, grad_own, False)
    pre_grad = back * head_ref[...] * curve_ref[...]
    cat_p[...] = shifted(pre_grad.astype(jnp.bfloat16))
    small_mine[...] = jnp.zeros_like(small_mine)
    small_mine[pl.ds(0, 1)] = jnp.sum(pre_grad, axis=0, keepdims=True)
    small_mine[pl.ds(1, 1)] = jnp.sum(back * slope_ref[...], axis=0, keepdims=True)

    pair, orders, rest = plan
    parts, shares, taps = total.shape[:3]
    lanes = land.shape[-1]
    split = chans // lanes
    half = shares // pair[2]
    units = chans // SUB

    def place_in(group):
        axis, stride, size = group
        return lax.rem(me[axis] // stride, size)

    def peer(group, step):
        axis, stride, size = group
        mine = place_in(group)
        other = lax.rem(mine + step, size)
        return other, device(**{axis: me[axis] + (other - mine) * stride})

    def pair_copy(a):
        other, target = peer(pair, 1)
        here = pl.ds(a * split, split)
        return pltpu.make_async_remote_copy(
            src_ref=total.at[here, pl.ds(other * half, half)], dst_ref=land_pair.at[here],
            send_sem=pair_send.at[a], recv_sem=pair_recv.at[a],
            device_id=target, device_id_type=MESH,
        )

    def correlate(a):
        def step(b, carry):
            dims = (((0,), (0,)), ((), ()))
            first = lax.dot_general(
                grad_pad[a : a + frames, b].reshape(count, chans), cat_s[...], dims,
                preferred_element_type=jnp.float32,
            )
            second = lax.dot_general(
                clip_pad[a : a + frames, b].reshape(count, chans), cat_p[...], dims,
                preferred_element_type=jnp.float32,
            )
            both = penalty_weight * first + second
            for d in range(TAPS):
                for p in range(split):
                    at = d * chans + p * lanes
                    total[a * split + p, :, b * TAPS + d] = both[:, at : at + lanes].reshape(
                        units, SUB, lanes
                    )
            return carry

        lax.fori_loop(0, TAPS, step, 0)
        if pair[2] > 1:
            pair_copy(a).start()

    def finish_pair(a):
        if pair[2] == 1:
            return
        mine = place_in(pair) * half
        pair_copy(a).wait()

        def add(step, carry):
            for p in range(a * split, (a + 1) * split):
                total[p, mine + step] = total[p, mine + step] + land_pair[p, step]
            return carry

        lax.fori_loop(0, half, add, 0)

    def encode(value):
        top = (jnp.max(jnp.abs(value), axis=0) * 1.01 + 1e-30).astype(jnp.bfloat16)
        rate = SPAN / top.astype(jnp.float32)
        return jnp.exp2(value * rate[None]).astype(jnp.bfloat16), top

    sems = {"part": 0, "gath": 0, "land": 0}

    def scatter_start(p, group, base, size, whole=False):
        share = size if whole else size // group[2]
        copies = []
        for step in range(1, group[2]):
            other, target = peer(group, step)
            origin = base if whole else base + other * share
            at = sems["land"]

            def fill(k, carry):
                value, top = encode(total[p, origin + k])
                code[at + k, pl.ds(0, taps)] = value
                code[at + k, taps] = top
                return carry

            lax.fori_loop(0, share, fill, 0)
            copy = pltpu.make_async_remote_copy(
                src_ref=code.at[pl.ds(at, share)], dst_ref=land.at[pl.ds(at, share)],
                send_sem=part_send.at[sems["part"]], recv_sem=part_recv.at[sems["part"]],
                device_id=target, device_id_type=MESH,
            )
            copy.start()
            copies.append((copy, at))
            sems["land"] += share
            sems["part"] += 1
        return copies, base if whole else base + place_in(group) * share, share

    def scatter_end(p, copies, base, share):
        for copy, _ in copies:
            copy.wait()
        if not copies:
            return

        def add(step, carry):
            value = total[p, base + step]
            for _, at in copies:
                value = value + decode(land[at + step], taps)
            total[p, base + step] = value
            return carry

        lax.fori_loop(0, share, add, 0)

    def gather_start(p, group, base, size):
        copies = []
        for step in range(1, group[2]):
            _, target = peer(group, step)
            block = full.at[p, pl.ds(base, size)]
            copy = pltpu.make_async_remote_copy(
                src_ref=block, dst_ref=block,
                send_sem=gath_send.at[sems["gath"]], recv_sem=gath_recv.at[sems["gath"]],
                device_id=target, device_id_type=MESH,
            )
            copy.start()
            copies.append(copy)
            sems["gath"] += 1
        return copies

    base = place_in(pair) * half
    state = [(base, half)] * parts
    trail = [[] for _ in range(parts)]
    started = [None] * parts
    depth = len(orders[0])

    def small_start(number, group, at):
        copies = []
        for step in range(1, group[2]):
            _, target = peer(group, step)
            copy = pltpu.make_async_remote_copy(
                src_ref=small_mine.at[pl.ds(number * SUB, SUB)],
                dst_ref=small_land.at[pl.ds(at * SUB, SUB)],
                send_sem=small_send.at[at], recv_sem=small_recv.at[at],
                device_id=target, device_id_type=MESH,
            )
            copy.start()
            copies.append((copy, at))
            at += 1
        return copies

    def small_end(number, copies):
        value = small_mine[pl.ds(number * SUB, SUB)]
        for copy, _ in copies:
            copy.wait()
        for _, slot in copies:
            value = value + small_land[pl.ds(slot * SUB, SUB)]
        small_mine[pl.ds((number + 1) * SUB, SUB)] = value

    def scatter(p, level):
        if level < depth:
            trail[p].append(state[p])
            started[p] = scatter_start(p, orders[p][level], *state[p])
        else:
            started[p] = scatter_start(p, rest[level - depth], *state[p], True)

    def end_scatter(p):
        copies, base, share = started[p]
        scatter_end(p, copies, base, share)
        state[p] = (base, share)

    small_groups = (pair, *orders[0], *rest)
    small_at = 0
    for a in range(TAPS):
        correlate(a)
        if a == 0:
            small = small_start(0, small_groups[0], small_at)
            small_at += len(small)
        else:
            finish_pair(a - 1)
            for p in range((a - 1) * split, a * split):
                scatter(p, 0)
    small_end(0, small)
    finish_pair(TAPS - 1)
    for p in range(parts - split, parts):
        scatter(p, 0)
    levels = depth + len(rest)
    for level in range(1, levels + 1):
        small = small_start(level, small_groups[level], small_at)
        small_at += len(small)
        for p in range(parts):
            end_scatter(p)
            if level < levels:
                scatter(p, level)
                continue
            base, size = state[p]

            def keep(k, carry):
                value, top = encode(total[p, base + k])
                full[p, base + k, pl.ds(0, taps)] = value
                full[p, base + k, taps] = top
                return carry

            lax.fori_loop(0, size, keep, 0)
            started[p] = gather_start(p, orders[p][depth - 1], *state[p])
        small_end(level, small)
    for k in range(2):
        small_refs[k][...] = small_mine[pl.ds((levels + 1) * SUB + k, 1)]
    for level in reversed(range(depth)):
        for p in range(parts):
            for copy in started[p]:
                copy.wait()
            state[p] = trail[p][level]
            group = orders[p][level - 1] if level else pair
            started[p] = gather_start(p, group, *state[p])
    outs = []
    for p in range(parts):
        for copy in started[p]:
            copy.wait()
        copy = pltpu.make_async_copy(full.at[p], out_ref.at[p], out_sem.at[p])
        copy.start()
        outs.append(copy)
    for copy in outs:
        copy.wait()


def decode(block, taps):
    unit = block[taps].astype(jnp.float32) * (1.0 / (SPAN * math.log(2.0)))
    return jnp.log(block[:taps].astype(jnp.float32)) * unit[None]


def decode_kernel(code_ref, bias_ref, head_ref, out_ref, bias_out, head_out):
    parts, shares, blocks, _, lanes = code_ref.shape
    taps = blocks - 1
    split = parts // TAPS
    for p in range(parts):
        at, lane = p // split * taps, p % split * lanes
        for k in range(shares):
            out_ref[at : at + taps, k, :, lane : lane + lanes] = decode(code_ref[p, k], taps)
    bias_out[...] = bias_ref[...]
    head_out[...] = head_ref[...]


def per_device(sizes, clips, weight, bias, head):
    _, frames, _, cols, chans = clips.shape
    count = frames * cols
    split = 2
    taps, shares, parts = TAPS**2, chans // SUB, TAPS * split
    lanes = chans // split
    plan = make_plan(sizes, shares)
    pair, orders, rest = plan
    half = shares // pair[2]
    small_n = sum(g[2] - 1 for g in (pair,) + orders[0] + rest)
    land = parts_n = gath_n = 0
    for order in orders:
        size = half
        for group in order:
            land += size // group[2] * (group[2] - 1)
            size //= group[2]
            parts_n += group[2] - 1
        for group in rest:
            land += size * (group[2] - 1)
            parts_n += group[2] - 1
        gath_n += sum(g[2] - 1 for g in order) + pair[2] - 1
    pad = pltpu.VMEM((frames + 2, 3, cols, chans), jnp.bfloat16)
    field = pltpu.VMEM((count, chans), jnp.float32)
    coded = pltpu.VMEM((max(land, 1), taps + 1, SUB, lanes), jnp.bfloat16)
    dma = pltpu.SemaphoreType.DMA
    vmem = pl.BlockSpec(memory_space=pltpu.VMEM)
    hbm = pl.BlockSpec(memory_space=pl.ANY)
    row = jax.ShapeDtypeStruct((1, chans), jnp.float32)
    code, *small = pl.pallas_call(
        functools.partial(kernel, sizes, plan),
        out_shape=(
            jax.ShapeDtypeStruct((parts, shares, taps + 1, SUB, lanes), jnp.bfloat16),
            row, row,
        ),
        in_specs=[hbm, hbm, vmem, vmem],
        out_specs=(hbm, vmem, vmem),
        scratch_shapes=[
            pltpu.VMEM((TAPS**3, chans, chans), jnp.bfloat16),
            pad, pad, pad,
            pltpu.VMEM((TAPS, count, chans), jnp.float32),
            field, field,
            pltpu.VMEM((count, TAPS * chans), jnp.bfloat16),
            pltpu.VMEM((count, TAPS * chans), jnp.bfloat16),
            pltpu.VMEM((parts, shares, taps, SUB, lanes), jnp.float32),
            pltpu.VMEM((parts, half, taps, SUB, lanes), jnp.float32),
            coded, coded,
            pltpu.VMEM((parts, shares, taps + 1, SUB, lanes), jnp.bfloat16),
            pltpu.VMEM(((len(rest) + 6) * SUB, chans), jnp.float32),
            pltpu.VMEM((max(small_n, 1) * SUB, chans), jnp.float32),
            dma((2,)), dma((24,)), dma((24,)), dma((TAPS,)), dma((TAPS,)),
            dma((max(parts_n, 1),)), dma((max(parts_n, 1),)),
            dma((max(gath_n, 1),)), dma((max(gath_n, 1),)),
            dma((max(small_n, 1),)), dma((max(small_n, 1),)), dma((parts,)),
        ],
        compiler_params=pltpu.CompilerParams(
            collective_id=0, has_side_effects=True, vmem_limit_bytes=60 * 1024 * 1024
        ),
    )(
        clips.reshape(frames, cols, chans),
        weight.reshape(TAPS**3, chans, chans),
        bias.reshape(1, chans),
        head.reshape(1, chans),
    )
    step = math.gcd(shares, 4)
    short = pl.BlockSpec((1, chans), lambda i: (0, 0))
    grad_weight, grad_bias, grad_head = pl.pallas_call(
        decode_kernel,
        out_shape=(jax.ShapeDtypeStruct((TAPS**3, shares, SUB, chans), jnp.float32), row, row),
        grid=(shares // step,),
        in_specs=[
            pl.BlockSpec((parts, step, taps + 1, SUB, lanes), lambda i: (0, i, 0, 0, 0)),
            short, short,
        ],
        out_specs=(
            pl.BlockSpec((TAPS**3, step, SUB, chans), lambda i: (0, i, 0, 0)), short, short
        ),
    )(code, *small)
    grad_weight = grad_weight.reshape(TAPS, TAPS, TAPS, chans, chans)
    return grad_weight, grad_bias.reshape(chans), grad_head.reshape(chans)


def solution(mesh):
    sizes = tuple(mesh.shape[axis] for axis in ("dp", "tm", "rows"))
    return jax.shard_map(
        functools.partial(per_device, sizes),
        mesh=mesh,
        in_specs=(P("dp", "tm", "rows", None, None), P(), P(), P()),
        out_specs=(P(), P(), P()),
        check_vma=False,
    )
```

```python
import functools
import math

import jax
import jax.numpy as jnp
from jax import lax
from jax.experimental import pallas as pl
from jax.experimental.pallas import tpu as pltpu
from jax.sharding import PartitionSpec as P

penalty_weight = 0.01
MESH = pl.DeviceIdType.MESH
SUB = 8
TAPS = 3
SPAN = 120.0


def make_plan(sizes, shares):
    dp, tm, rows = sizes
    cuts, rest, left = [], [], shares
    near = 2 if rows % 2 == 0 else 1
    for axis, stride, count in (("rows", 1, near), ("rows", near, rows // near), ("dp", 1, dp), ("tm", 1, tm)):
        cut = 1
        while count % (2 * cut) == 0 and left % (2 * cut) == 0:
            cut *= 2
        left //= cut
        cuts.append((axis, stride, cut))
        rest.append((axis, stride * cut, count // cut))
    pair, far, depth, line = cuts
    rest = tuple(group for group in rest if group[2] > 1)
    across, along, ahead = (far, depth, line), (depth, far, line), (line, depth, far)
    between = (depth, line, far)
    return pair, (ahead, along, across, between, across, along), rest


def kernel(
    sizes, plan, clips_ref, weight_ref, bias_ref, head_ref,
    out_ref, bias_out, head_out,
    w_ref, clip_pad, score_pad, grad_pad, acc, slope_ref, curve_ref, cat_s, cat_p, total,
    land_pair, code, land, full, small_mine, small_land,
    local_sem, halo_send, halo_recv, pair_send, pair_recv, part_send, part_recv, gath_send, gath_recv,
    small_send, small_recv, out_sem,
):
    small_refs = (bias_out, head_out)
    dp, tm, rows = sizes
    frames, cols, chans = clips_ref.shape
    count = frames * cols
    me = {"dp": lax.axis_index("dp"), "tm": lax.axis_index("tm"), "rows": lax.axis_index("rows")}

    def device(**moved):
        place = dict(me, **moved)
        return (place["dp"], place["tm"], place["rows"])

    weight_copy = pltpu.make_async_copy(weight_ref, w_ref, local_sem.at[0])
    weight_copy.start()
    clip_copy = pltpu.make_async_copy(
        clips_ref, clip_pad.at[pl.ds(1, frames), 1], local_sem.at[1]
    )
    clip_copy.start()
    for pad in (clip_pad, score_pad, grad_pad):
        pad[:, 0] = jnp.zeros((frames + 2, cols, chans), pad.dtype)
        pad[:, 2] = jnp.zeros((frames + 2, cols, chans), pad.dtype)
        pad[0, 1] = jnp.zeros((cols, chans), pad.dtype)
        pad[frames + 1, 1] = jnp.zeros((cols, chans), pad.dtype)

    barrier = pltpu.get_barrier_semaphore()
    flat = me["tm"] * rows + me["rows"]
    plane = tm * rows

    def greet(step, carry):
        other = lax.rem(flat + step, plane)
        pl.semaphore_signal(
            barrier, inc=1, device_id=device(tm=other // rows, rows=lax.rem(other, rows)),
            device_id_type=MESH,
        )
        return carry

    lax.fori_loop(1, plane, greet, 0)
    for step in range(1, dp):
        pl.semaphore_signal(
            barrier, inc=1, device_id=device(dp=lax.rem(me["dp"] + step, dp)), device_id_type=MESH
        )
    pl.semaphore_wait(barrier, plane - 1 + dp - 1)

    moves = [(t, r) for t in (-1, 0, 1) for r in (-1, 0, 1) if (t, r) != (0, 0)]

    def inside(t, r):
        ok = None
        for axis, step, size in (("tm", t, tm), ("rows", r, rows)):
            if step:
                cond = me[axis] > 0 if step < 0 else me[axis] < size - 1
                ok = cond if ok is None else jnp.logical_and(ok, cond)
        return ok

    def halo_copy(which, pad, source, t, r):
        slot = which * len(moves) + moves.index((t, r))
        if t == 0:
            here, there = pl.ds(0, frames), pl.ds(1, frames)
        elif t > 0:
            here, there = pl.ds(frames - 1, 1), pl.ds(0, 1)
        else:
            here, there = pl.ds(0, 1), pl.ds(frames + 1, 1)
        return pltpu.make_async_remote_copy(
            src_ref=source.at[here], dst_ref=pad.at[there, 1 - r],
            send_sem=halo_send.at[slot], recv_sem=halo_recv.at[slot],
            device_id=device(tm=me["tm"] + t, rows=me["rows"] + r), device_id_type=MESH,
        )

    def halo_start(which, pad, source):
        for t, r in moves:
            @pl.when(inside(t, r))
            def _():
                halo_copy(which, pad, source, t, r).start()

    def halo_wait(which, pad, source, level):
        for t, r in moves:
            if (t == 0) != level:
                continue

            @pl.when(inside(t, r))
            def _():
                halo_copy(which, pad, source, t, r).wait_send()

            @pl.when(inside(-t, -r))
            def _():
                halo_copy(which, pad, source, t, r).wait_recv()

    column = lax.rem(lax.broadcasted_iota(jnp.int32, (count, chans), 0), cols)

    def earlier(value):
        return jnp.where(column == 0, 0.0, pltpu.roll(value, 1, 0))

    def later(value):
        return jnp.where(column == cols - 1, 0.0, pltpu.roll(value, count - 1, 0))

    def conv(which, pad, source, transpose):
        def step(a):
            base = (TAPS - 1 - a) if transpose else a
            pieces = [
                pad[pl.ds(base, frames), (TAPS - 1 - b) if transpose else b].reshape(count, chans)
                for b in range(TAPS)
            ]
            left = jnp.concatenate(pieces, axis=1)
            for d in range(TAPS):
                taps = [w_ref[(a * TAPS + b) * TAPS + d] for b in range(TAPS)]
                if transpose:
                    part = lax.dot_general(
                        left, jnp.concatenate(taps, axis=1), (((1,), (1,)), ((), ())),
                        preferred_element_type=jnp.float32,
                    )
                else:
                    part = jnp.dot(
                        left, jnp.concatenate(taps, axis=0), preferred_element_type=jnp.float32
                    )
                acc[d] = part if a == 1 else acc[d] + part

        halo_wait(which, pad, source, True)
        step(1)
        halo_wait(which, pad, source, False)
        step(0)
        step(2)
        if transpose:
            return later(acc[0]) + acc[1] + earlier(acc[2])
        return earlier(acc[0]) + acc[1] + later(acc[2])

    def shifted(value):
        value = value.astype(jnp.float32)
        return jnp.concatenate(
            [later(value), value, earlier(value)], axis=1
        ).astype(jnp.bfloat16)

    halo_start(0, clip_pad, clips_ref)
    clip_copy.wait()
    weight_copy.wait()
    pre = conv(0, clip_pad, clips_ref, False) + bias_ref[...]
    sig = jax.nn.sigmoid(pre)
    slope = sig * (1.0 + pre * (1.0 - sig))
    slope_ref[...] = slope
    curve_ref[...] = sig * (1.0 - sig) * (2.0 + pre * (1.0 - 2.0 * sig))
    score = (head_ref[...] * slope).astype(jnp.bfloat16)
    score_pad[pl.ds(1, frames), 1] = score.reshape(frames, cols, chans)
    score_own = score_pad.at[pl.ds(1, frames), 1]
    cat_s[...] = shifted(score)
    halo_start(1, score_pad, score_own)

    input_grad = conv(1, score_pad, score_own, True).astype(jnp.bfloat16)
    grad_pad[pl.ds(1, frames), 1] = input_grad.reshape(frames, cols, chans)
    grad_own = grad_pad.at[pl.ds(1, frames), 1]
    halo_start(2, grad_pad, grad_own)

    back = penalty_weight * conv(2, grad_pad, grad_own, False)
    pre_grad = back * head_ref[...] * curve_ref[...]
    cat_p[...] = shifted(pre_grad.astype(jnp.bfloat16))
    small_mine[...] = jnp.zeros_like(small_mine)
    small_mine[pl.ds(0, 1)] = jnp.sum(pre_grad, axis=0, keepdims=True)
    small_mine[pl.ds(1, 1)] = jnp.sum(back * slope_ref[...], axis=0, keepdims=True)

    pair, orders, rest = plan
    parts, shares, taps = total.shape[:3]
    lanes = land.shape[-1]
    split = chans // lanes
    half = shares // pair[2]
    units = chans // SUB

    def place_in(group):
        axis, stride, size = group
        return lax.rem(me[axis] // stride, size)

    def peer(group, step):
        axis, stride, size = group
        mine = place_in(group)
        other = lax.rem(mine + step, size)
        return other, device(**{axis: me[axis] + (other - mine) * stride})

    def pair_copy(a):
        other, target = peer(pair, 1)
        here = pl.ds(a * split, split)
        return pltpu.make_async_remote_copy(
            src_ref=total.at[here, pl.ds(other * half, half)], dst_ref=land_pair.at[here],
            send_sem=pair_send.at[a], recv_sem=pair_recv.at[a],
            device_id=target, device_id_type=MESH,
        )

    def correlate(a):
        def step(b, carry):
            dims = (((0,), (0,)), ((), ()))
            first = lax.dot_general(
                grad_pad[a : a + frames, b].reshape(count, chans), cat_s[...], dims,
                preferred_element_type=jnp.float32,
            )
            second = lax.dot_general(
                clip_pad[a : a + frames, b].reshape(count, chans), cat_p[...], dims,
                preferred_element_type=jnp.float32,
            )
            both = penalty_weight * first + second
            for d in range(TAPS):
                for p in range(split):
                    at = d * chans + p * lanes
                    total[a * split + p, :, b * TAPS + d] = both[:, at : at + lanes].reshape(
                        units, SUB, lanes
                    )
            return carry

        lax.fori_loop(0, TAPS, step, 0)
        if pair[2] > 1:
            pair_copy(a).start()

    def finish_pair(a):
        if pair[2] == 1:
            return
        mine = place_in(pair) * half
        pair_copy(a).wait()

        def add(step, carry):
            for p in range(a * split, (a + 1) * split):
                total[p, mine + step] = total[p, mine + step] + land_pair[p, step]
            return carry

        lax.fori_loop(0, half, add, 0)

    def encode(value):
        top = (jnp.max(jnp.abs(value), axis=0) * 1.01 + 1e-30).astype(jnp.bfloat16)
        rate = SPAN / top.astype(jnp.float32)
        return jnp.exp2(value * rate[None]).astype(jnp.bfloat16), top

    sems = {"part": 0, "gath": 0, "land": 0}

    def scatter_start(p, group, base, size, whole=False):
        share = size if whole else size // group[2]
        copies = []
        for step in range(1, group[2]):
            other, target = peer(group, step)
            origin = base if whole else base + other * share
            at = sems["land"]

            def fill(k, carry):
                value, top = encode(total[p, origin + k])
                code[at + k, pl.ds(0, taps)] = value
                code[at + k, taps] = top
                return carry

            lax.fori_loop(0, share, fill, 0)
            copy = pltpu.make_async_remote_copy(
                src_ref=code.at[pl.ds(at, share)], dst_ref=land.at[pl.ds(at, share)],
                send_sem=part_send.at[sems["part"]], recv_sem=part_recv.at[sems["part"]],
                device_id=target, device_id_type=MESH,
            )
            copy.start()
            copies.append((copy, at))
            sems["land"] += share
            sems["part"] += 1
        return copies, base if whole else base + place_in(group) * share, share

    def scatter_end(p, copies, base, share):
        for copy, _ in copies:
            copy.wait()
        if not copies:
            return

        def add(step, carry):
            value = total[p, base + step]
            for _, at in copies:
                value = value + decode(land[at + step], taps)
            total[p, base + step] = value
            return carry

        lax.fori_loop(0, share, add, 0)

    def gather_start(p, group, base, size):
        copies = []
        for step in range(1, group[2]):
            _, target = peer(group, step)
            block = full.at[p, pl.ds(base, size)]
            copy = pltpu.make_async_remote_copy(
                src_ref=block, dst_ref=block,
                send_sem=gath_send.at[sems["gath"]], recv_sem=gath_recv.at[sems["gath"]],
                device_id=target, device_id_type=MESH,
            )
            copy.start()
            copies.append(copy)
            sems["gath"] += 1
        return copies

    base = place_in(pair) * half
    state = [(base, half)] * parts
    trail = [[] for _ in range(parts)]
    started = [None] * parts
    depth = len(orders[0])

    def small_start(number, group, at):
        copies = []
        for step in range(1, group[2]):
            _, target = peer(group, step)
            copy = pltpu.make_async_remote_copy(
                src_ref=small_mine.at[pl.ds(number * SUB, SUB)],
                dst_ref=small_land.at[pl.ds(at * SUB, SUB)],
                send_sem=small_send.at[at], recv_sem=small_recv.at[at],
                device_id=target, device_id_type=MESH,
            )
            copy.start()
            copies.append((copy, at))
            at += 1
        return copies

    def small_end(number, copies):
        value = small_mine[pl.ds(number * SUB, SUB)]
        for copy, _ in copies:
            copy.wait()
        for _, slot in copies:
            value = value + small_land[pl.ds(slot * SUB, SUB)]
        small_mine[pl.ds((number + 1) * SUB, SUB)] = value

    def scatter(p, level):
        if level < depth:
            trail[p].append(state[p])
            started[p] = scatter_start(p, orders[p][level], *state[p])
        else:
            started[p] = scatter_start(p, rest[level - depth], *state[p], True)

    def end_scatter(p):
        copies, base, share = started[p]
        scatter_end(p, copies, base, share)
        state[p] = (base, share)

    small_groups = (pair, *orders[0], *rest)
    small_at = 0
    for a in range(TAPS):
        correlate(a)
        if a == 0:
            small = small_start(0, small_groups[0], small_at)
            small_at += len(small)
        else:
            finish_pair(a - 1)
            for p in range((a - 1) * split, a * split):
                scatter(p, 0)
    small_end(0, small)
    finish_pair(TAPS - 1)
    for p in range(parts - split, parts):
        scatter(p, 0)
    levels = depth + len(rest)
    for level in range(1, levels + 1):
        small = small_start(level, small_groups[level], small_at)
        small_at += len(small)
        for p in range(parts):
            end_scatter(p)
            if level < levels:
                scatter(p, level)
                continue
            base, size = state[p]

            def keep(k, carry):
                value, top = encode(total[p, base + k])
                full[p, base + k, pl.ds(0, taps)] = value
                full[p, base + k, taps] = top
                return carry

            lax.fori_loop(0, size, keep, 0)
            started[p] = gather_start(p, orders[p][depth - 1], *state[p])
        small_end(level, small)
    for k in range(2):
        small_refs[k][...] = small_mine[pl.ds((levels + 1) * SUB + k, 1)]
    for level in reversed(range(depth)):
        for p in range(parts):
            for copy in started[p]:
                copy.wait()
            state[p] = trail[p][level]
            group = orders[p][level - 1] if level else pair
            started[p] = gather_start(p, group, *state[p])
    outs = []
    for p in range(parts):
        for copy in started[p]:
            copy.wait()
        copy = pltpu.make_async_copy(full.at[p], out_ref.at[p], out_sem.at[p])
        copy.start()
        outs.append(copy)
    for copy in outs:
        copy.wait()


def decode(block, taps):
    unit = block[taps].astype(jnp.float32) * (1.0 / (SPAN * math.log(2.0)))
    return jnp.log(block[:taps].astype(jnp.float32)) * unit[None]


def decode_kernel(code_ref, bias_ref, head_ref, out_ref, bias_out, head_out):
    parts, shares, blocks, _, lanes = code_ref.shape
    taps = blocks - 1
    split = parts // TAPS
    for p in range(parts):
        at, lane = p // split * taps, p % split * lanes
        for k in range(shares):
            out_ref[at : at + taps, k, :, lane : lane + lanes] = decode(code_ref[p, k], taps)
    bias_out[...] = bias_ref[...]
    head_out[...] = head_ref[...]


def per_device(sizes, clips, weight, bias, head):
    _, frames, _, cols, chans = clips.shape
    count = frames * cols
    split = 2
    taps, shares, parts = TAPS**2, chans // SUB, TAPS * split
    lanes = chans // split
    plan = make_plan(sizes, shares)
    pair, orders, rest = plan
    half = shares // pair[2]
    small_n = sum(g[2] - 1 for g in (pair,) + orders[0] + rest)
    land = parts_n = gath_n = 0
    for order in orders:
        size = half
        for group in order:
            land += size // group[2] * (group[2] - 1)
            size //= group[2]
            parts_n += group[2] - 1
        for group in rest:
            land += size * (group[2] - 1)
            parts_n += group[2] - 1
        gath_n += sum(g[2] - 1 for g in order) + pair[2] - 1
    pad = pltpu.VMEM((frames + 2, 3, cols, chans), jnp.bfloat16)
    field = pltpu.VMEM((count, chans), jnp.float32)
    coded = pltpu.VMEM((max(land, 1), taps + 1, SUB, lanes), jnp.bfloat16)
    dma = pltpu.SemaphoreType.DMA
    vmem = pl.BlockSpec(memory_space=pltpu.VMEM)
    hbm = pl.BlockSpec(memory_space=pl.ANY)
    row = jax.ShapeDtypeStruct((1, chans), jnp.float32)
    code, *small = pl.pallas_call(
        functools.partial(kernel, sizes, plan),
        out_shape=(
            jax.ShapeDtypeStruct((parts, shares, taps + 1, SUB, lanes), jnp.bfloat16),
            row, row,
        ),
        in_specs=[hbm, hbm, vmem, vmem],
        out_specs=(hbm, vmem, vmem),
        scratch_shapes=[
            pltpu.VMEM((TAPS**3, chans, chans), jnp.bfloat16),
            pad, pad, pad,
            pltpu.VMEM((TAPS, count, chans), jnp.float32),
            field, field,
            pltpu.VMEM((count, TAPS * chans), jnp.bfloat16),
            pltpu.VMEM((count, TAPS * chans), jnp.bfloat16),
            pltpu.VMEM((parts, shares, taps, SUB, lanes), jnp.float32),
            pltpu.VMEM((parts, half, taps, SUB, lanes), jnp.float32),
            coded, coded,
            pltpu.VMEM((parts, shares, taps + 1, SUB, lanes), jnp.bfloat16),
            pltpu.VMEM(((len(rest) + 6) * SUB, chans), jnp.float32),
            pltpu.VMEM((max(small_n, 1) * SUB, chans), jnp.float32),
            dma((2,)), dma((24,)), dma((24,)), dma((TAPS,)), dma((TAPS,)),
            dma((max(parts_n, 1),)), dma((max(parts_n, 1),)),
            dma((max(gath_n, 1),)), dma((max(gath_n, 1),)),
            dma((max(small_n, 1),)), dma((max(small_n, 1),)), dma((parts,)),
        ],
        compiler_params=pltpu.CompilerParams(
            collective_id=0, has_side_effects=True, vmem_limit_bytes=60 * 1024 * 1024
        ),
    )(
        clips.reshape(frames, cols, chans),
        weight.reshape(TAPS**3, chans, chans),
        bias.reshape(1, chans),
        head.reshape(1, chans),
    )
    step = math.gcd(shares, 8)
    short = pl.BlockSpec((1, chans), lambda i: (0, 0))
    grad_weight, grad_bias, grad_head = pl.pallas_call(
        decode_kernel,
        out_shape=(jax.ShapeDtypeStruct((TAPS**3, shares, SUB, chans), jnp.float32), row, row),
        grid=(shares // step,),
        in_specs=[
            pl.BlockSpec((parts, step, taps + 1, SUB, lanes), lambda i: (0, i, 0, 0, 0)),
            short, short,
        ],
        out_specs=(
            pl.BlockSpec((TAPS**3, step, SUB, chans), lambda i: (0, i, 0, 0)), short, short
        ),
    )(code, *small)
    grad_weight = grad_weight.reshape(TAPS, TAPS, TAPS, chans, chans)
    return grad_weight, grad_bias.reshape(chans), grad_head.reshape(chans)


def solution(mesh):
    sizes = tuple(mesh.shape[axis] for axis in ("dp", "tm", "rows"))
    return jax.shard_map(
        functools.partial(per_device, sizes),
        mesh=mesh,
        in_specs=(P("dp", "tm", "rows", None, None), P(), P(), P()),
        out_specs=(P(), P(), P()),
        check_vma=False,
    )
```

```python
import functools
import math

import jax
import jax.numpy as jnp
from jax import lax
from jax.experimental import pallas as pl
from jax.experimental.pallas import tpu as pltpu
from jax.sharding import PartitionSpec as P

penalty_weight = 0.01
MESH = pl.DeviceIdType.MESH
SUB = 8
TAPS = 3
SPAN = 120.0


def make_plan(sizes, shares):
    dp, tm, rows = sizes
    cuts, rest, left = [], [], shares
    near = 2 if rows % 2 == 0 else 1
    for axis, stride, count in (("rows", 1, near), ("rows", near, rows // near), ("dp", 1, dp), ("tm", 1, tm)):
        cut = 1
        while count % (2 * cut) == 0 and left % (2 * cut) == 0:
            cut *= 2
        left //= cut
        cuts.append((axis, stride, cut))
        rest.append((axis, stride * cut, count // cut))
    pair, far, depth, line = cuts
    rest = tuple(group for group in rest if group[2] > 1)
    across, along, ahead = (far, depth, line), (depth, far, line), (line, depth, far)
    between = (depth, line, far)
    return pair, (ahead, across, along, between, across, along), rest


def kernel(
    sizes, plan, clips_ref, weight_ref, bias_ref, head_ref,
    out_ref, bias_out, head_out,
    w_ref, clip_pad, score_pad, grad_pad, acc, slope_ref, curve_ref, cat_s, cat_p, total,
    land_pair, code, land, full, small_mine, small_land,
    local_sem, halo_send, halo_recv, pair_send, pair_recv, part_send, part_recv, gath_send, gath_recv,
    small_send, small_recv, out_sem,
):
    small_refs = (bias_out, head_out)
    dp, tm, rows = sizes
    frames, cols, chans = clips_ref.shape
    count = frames * cols
    me = {"dp": lax.axis_index("dp"), "tm": lax.axis_index("tm"), "rows": lax.axis_index("rows")}

    def device(**moved):
        place = dict(me, **moved)
        return (place["dp"], place["tm"], place["rows"])

    weight_copy = pltpu.make_async_copy(weight_ref, w_ref, local_sem.at[0])
    weight_copy.start()
    clip_copy = pltpu.make_async_copy(
        clips_ref, clip_pad.at[pl.ds(1, frames), 1], local_sem.at[1]
    )
    clip_copy.start()
    for pad in (clip_pad, score_pad, grad_pad):
        pad[:, 0] = jnp.zeros((frames + 2, cols, chans), pad.dtype)
        pad[:, 2] = jnp.zeros((frames + 2, cols, chans), pad.dtype)
        pad[0, 1] = jnp.zeros((cols, chans), pad.dtype)
        pad[frames + 1, 1] = jnp.zeros((cols, chans), pad.dtype)

    barrier = pltpu.get_barrier_semaphore()
    flat = me["tm"] * rows + me["rows"]
    plane = tm * rows

    def greet(step, carry):
        other = lax.rem(flat + step, plane)
        pl.semaphore_signal(
            barrier, inc=1, device_id=device(tm=other // rows, rows=lax.rem(other, rows)),
            device_id_type=MESH,
        )
        return carry

    lax.fori_loop(1, plane, greet, 0)
    for step in range(1, dp):
        pl.semaphore_signal(
            barrier, inc=1, device_id=device(dp=lax.rem(me["dp"] + step, dp)), device_id_type=MESH
        )
    pl.semaphore_wait(barrier, plane - 1 + dp - 1)

    moves = [(t, r) for t in (-1, 0, 1) for r in (-1, 0, 1) if (t, r) != (0, 0)]

    def inside(t, r):
        ok = None
        for axis, step, size in (("tm", t, tm), ("rows", r, rows)):
            if step:
                cond = me[axis] > 0 if step < 0 else me[axis] < size - 1
                ok = cond if ok is None else jnp.logical_and(ok, cond)
        return ok

    def halo_copy(which, pad, source, t, r):
        slot = which * len(moves) + moves.index((t, r))
        if t == 0:
            here, there = pl.ds(0, frames), pl.ds(1, frames)
        elif t > 0:
            here, there = pl.ds(frames - 1, 1), pl.ds(0, 1)
        else:
            here, there = pl.ds(0, 1), pl.ds(frames + 1, 1)
        return pltpu.make_async_remote_copy(
            src_ref=source.at[here], dst_ref=pad.at[there, 1 - r],
            send_sem=halo_send.at[slot], recv_sem=halo_recv.at[slot],
            device_id=device(tm=me["tm"] + t, rows=me["rows"] + r), device_id_type=MESH,
        )

    def halo_start(which, pad, source):
        for t, r in moves:
            @pl.when(inside(t, r))
            def _():
                halo_copy(which, pad, source, t, r).start()

    def halo_wait(which, pad, source, level):
        for t, r in moves:
            if (t == 0) != level:
                continue

            @pl.when(inside(t, r))
            def _():
                halo_copy(which, pad, source, t, r).wait_send()

            @pl.when(inside(-t, -r))
            def _():
                halo_copy(which, pad, source, t, r).wait_recv()

    column = lax.rem(lax.broadcasted_iota(jnp.int32, (count, chans), 0), cols)

    def earlier(value):
        return jnp.where(column == 0, 0.0, pltpu.roll(value, 1, 0))

    def later(value):
        return jnp.where(column == cols - 1, 0.0, pltpu.roll(value, count - 1, 0))

    def conv(which, pad, source, transpose):
        def step(a):
            base = (TAPS - 1 - a) if transpose else a
            pieces = [
                pad[pl.ds(base, frames), (TAPS - 1 - b) if transpose else b].reshape(count, chans)
                for b in range(TAPS)
            ]
            left = jnp.concatenate(pieces, axis=1)
            for d in range(TAPS):
                taps = [w_ref[(a * TAPS + b) * TAPS + d] for b in range(TAPS)]
                if transpose:
                    part = lax.dot_general(
                        left, jnp.concatenate(taps, axis=1), (((1,), (1,)), ((), ())),
                        preferred_element_type=jnp.float32,
                    )
                else:
                    part = jnp.dot(
                        left, jnp.concatenate(taps, axis=0), preferred_element_type=jnp.float32
                    )
                acc[d] = part if a == 1 else acc[d] + part

        halo_wait(which, pad, source, True)
        step(1)
        halo_wait(which, pad, source, False)
        step(0)
        step(2)
        if transpose:
            return later(acc[0]) + acc[1] + earlier(acc[2])
        return earlier(acc[0]) + acc[1] + later(acc[2])

    def shifted(value):
        value = value.astype(jnp.float32)
        return jnp.concatenate(
            [later(value), value, earlier(value)], axis=1
        ).astype(jnp.bfloat16)

    halo_start(0, clip_pad, clips_ref)
    clip_copy.wait()
    weight_copy.wait()
    pre = conv(0, clip_pad, clips_ref, False) + bias_ref[...]
    sig = jax.nn.sigmoid(pre)
    slope = sig * (1.0 + pre * (1.0 - sig))
    slope_ref[...] = slope
    curve_ref[...] = sig * (1.0 - sig) * (2.0 + pre * (1.0 - 2.0 * sig))
    score = (head_ref[...] * slope).astype(jnp.bfloat16)
    score_pad[pl.ds(1, frames), 1] = score.reshape(frames, cols, chans)
    score_own = score_pad.at[pl.ds(1, frames), 1]
    cat_s[...] = shifted(score)
    halo_start(1, score_pad, score_own)

    input_grad = conv(1, score_pad, score_own, True).astype(jnp.bfloat16)
    grad_pad[pl.ds(1, frames), 1] = input_grad.reshape(frames, cols, chans)
    grad_own = grad_pad.at[pl.ds(1, frames), 1]
    halo_start(2, grad_pad, grad_own)

    back = penalty_weight * conv(2, grad_pad, grad_own, False)
    pre_grad = back * head_ref[...] * curve_ref[...]
    cat_p[...] = shifted(pre_grad.astype(jnp.bfloat16))
    small_mine[...] = jnp.zeros_like(small_mine)
    small_mine[pl.ds(0, 1)] = jnp.sum(pre_grad, axis=0, keepdims=True)
    small_mine[pl.ds(1, 1)] = jnp.sum(back * slope_ref[...], axis=0, keepdims=True)

    pair, orders, rest = plan
    parts, shares, taps = total.shape[:3]
    lanes = land.shape[-1]
    split = chans // lanes
    half = shares // pair[2]
    units = chans // SUB

    def place_in(group):
        axis, stride, size = group
        return lax.rem(me[axis] // stride, size)

    def peer(group, step):
        axis, stride, size = group
        mine = place_in(group)
        other = lax.rem(mine + step, size)
        return other, device(**{axis: me[axis] + (other - mine) * stride})

    def pair_copy(a):
        other, target = peer(pair, 1)
        here = pl.ds(a * split, split)
        return pltpu.make_async_remote_copy(
            src_ref=total.at[here, pl.ds(other * half, half)], dst_ref=land_pair.at[here],
            send_sem=pair_send.at[a], recv_sem=pair_recv.at[a],
            device_id=target, device_id_type=MESH,
        )

    def correlate(a):
        def step(b, carry):
            dims = (((0,), (0,)), ((), ()))
            first = lax.dot_general(
                grad_pad[a : a + frames, b].reshape(count, chans), cat_s[...], dims,
                preferred_element_type=jnp.float32,
            )
            second = lax.dot_general(
                clip_pad[a : a + frames, b].reshape(count, chans), cat_p[...], dims,
                preferred_element_type=jnp.float32,
            )
            both = penalty_weight * first + second
            for d in range(TAPS):
                for p in range(split):
                    at = d * chans + p * lanes
                    total[a * split + p, :, b * TAPS + d] = both[:, at : at + lanes].reshape(
                        units, SUB, lanes
                    )
            return carry

        lax.fori_loop(0, TAPS, step, 0)
        if pair[2] > 1:
            pair_copy(a).start()

    def finish_pair(a):
        if pair[2] == 1:
            return
        mine = place_in(pair) * half
        pair_copy(a).wait()

        def add(step, carry):
            for p in range(a * split, (a + 1) * split):
                total[p, mine + step] = total[p, mine + step] + land_pair[p, step]
            return carry

        lax.fori_loop(0, half, add, 0)

    def encode(value):
        top = (jnp.max(jnp.abs(value), axis=0) * 1.01 + 1e-30).astype(jnp.bfloat16)
        rate = SPAN / top.astype(jnp.float32)
        return jnp.exp2(value * rate[None]).astype(jnp.bfloat16), top

    sems = {"part": 0, "gath": 0, "land": 0}

    def scatter_start(p, group, base, size, whole=False):
        share = size if whole else size // group[2]
        copies = []
        for step in range(1, group[2]):
            other, target = peer(group, step)
            origin = base if whole else base + other * share
            at = sems["land"]

            def fill(k, carry):
                value, top = encode(total[p, origin + k])
                code[at + k, pl.ds(0, taps)] = value
                code[at + k, taps] = top
                return carry

            lax.fori_loop(0, share, fill, 0)
            copy = pltpu.make_async_remote_copy(
                src_ref=code.at[pl.ds(at, share)], dst_ref=land.at[pl.ds(at, share)],
                send_sem=part_send.at[sems["part"]], recv_sem=part_recv.at[sems["part"]],
                device_id=target, device_id_type=MESH,
            )
            copy.start()
            copies.append((copy, at))
            sems["land"] += share
            sems["part"] += 1
        return copies, base if whole else base + place_in(group) * share, share

    def scatter_end(p, copies, base, share):
        for copy, _ in copies:
            copy.wait()
        if not copies:
            return

        def add(step, carry):
            value = total[p, base + step]
            for _, at in copies:
                value = value + decode(land[at + step], taps)
            total[p, base + step] = value
            return carry

        lax.fori_loop(0, share, add, 0)

    def gather_start(p, group, base, size):
        copies = []
        for step in range(1, group[2]):
            _, target = peer(group, step)
            block = full.at[p, pl.ds(base, size)]
            copy = pltpu.make_async_remote_copy(
                src_ref=block, dst_ref=block,
                send_sem=gath_send.at[sems["gath"]], recv_sem=gath_recv.at[sems["gath"]],
                device_id=target, device_id_type=MESH,
            )
            copy.start()
            copies.append(copy)
            sems["gath"] += 1
        return copies

    base = place_in(pair) * half
    state = [(base, half)] * parts
    trail = [[] for _ in range(parts)]
    started = [None] * parts
    depth = len(orders[0])

    def small_start(number, group, at):
        copies = []
        for step in range(1, group[2]):
            _, target = peer(group, step)
            copy = pltpu.make_async_remote_copy(
                src_ref=small_mine.at[pl.ds(number * SUB, SUB)],
                dst_ref=small_land.at[pl.ds(at * SUB, SUB)],
                send_sem=small_send.at[at], recv_sem=small_recv.at[at],
                device_id=target, device_id_type=MESH,
            )
            copy.start()
            copies.append((copy, at))
            at += 1
        return copies

    def small_end(number, copies):
        value = small_mine[pl.ds(number * SUB, SUB)]
        for copy, _ in copies:
            copy.wait()
        for _, slot in copies:
            value = value + small_land[pl.ds(slot * SUB, SUB)]
        small_mine[pl.ds((number + 1) * SUB, SUB)] = value

    def scatter(p, level):
        if level < depth:
            trail[p].append(state[p])
            started[p] = scatter_start(p, orders[p][level], *state[p])
        else:
            started[p] = scatter_start(p, rest[level - depth], *state[p], True)

    def end_scatter(p):
        copies, base, share = started[p]
        scatter_end(p, copies, base, share)
        state[p] = (base, share)

    small_groups = (pair, *orders[0], *rest)
    small_at = 0
    for a in range(TAPS):
        correlate(a)
        if a == 0:
            small = small_start(0, small_groups[0], small_at)
            small_at += len(small)
        else:
            finish_pair(a - 1)
            for p in range((a - 1) * split, a * split):
                scatter(p, 0)
    small_end(0, small)
    finish_pair(TAPS - 1)
    for p in range(parts - split, parts):
        scatter(p, 0)
    levels = depth + len(rest)
    for level in range(1, levels + 1):
        small = small_start(level, small_groups[level], small_at)
        small_at += len(small)
        for p in range(parts):
            end_scatter(p)
            if level < levels:
                scatter(p, level)
                continue
            base, size = state[p]

            def keep(k, carry):
                value, top = encode(total[p, base + k])
                full[p, base + k, pl.ds(0, taps)] = value
                full[p, base + k, taps] = top
                return carry

            lax.fori_loop(0, size, keep, 0)
            started[p] = gather_start(p, orders[p][depth - 1], *state[p])
        small_end(level, small)
    for k in range(2):
        small_refs[k][...] = small_mine[pl.ds((levels + 1) * SUB + k, 1)]
    for level in reversed(range(depth)):
        for p in range(parts):
            for copy in started[p]:
                copy.wait()
            state[p] = trail[p][level]
            group = orders[p][level - 1] if level else pair
            started[p] = gather_start(p, group, *state[p])
    outs = []
    for p in range(parts):
        for copy in started[p]:
            copy.wait()
        copy = pltpu.make_async_copy(full.at[p], out_ref.at[p], out_sem.at[p])
        copy.start()
        outs.append(copy)
    for copy in outs:
        copy.wait()


def decode(block, taps):
    unit = block[taps].astype(jnp.float32) * (1.0 / (SPAN * math.log(2.0)))
    return jnp.log(block[:taps].astype(jnp.float32)) * unit[None]


def decode_kernel(code_ref, bias_ref, head_ref, out_ref, bias_out, head_out):
    parts, shares, blocks, _, lanes = code_ref.shape
    taps = blocks - 1
    split = parts // TAPS
    for p in range(parts):
        at, lane = p // split * taps, p % split * lanes
        for k in range(shares):
            out_ref[at : at + taps, k, :, lane : lane + lanes] = decode(code_ref[p, k], taps)
    bias_out[...] = bias_ref[...]
    head_out[...] = head_ref[...]


def per_device(sizes, clips, weight, bias, head):
    _, frames, _, cols, chans = clips.shape
    count = frames * cols
    split = 2
    taps, shares, parts = TAPS**2, chans // SUB, TAPS * split
    lanes = chans // split
    plan = make_plan(sizes, shares)
    pair, orders, rest = plan
    half = shares // pair[2]
    small_n = sum(g[2] - 1 for g in (pair,) + orders[0] + rest)
    land = parts_n = gath_n = 0
    for order in orders:
        size = half
        for group in order:
            land += size // group[2] * (group[2] - 1)
            size //= group[2]
            parts_n += group[2] - 1
        for group in rest:
            land += size * (group[2] - 1)
            parts_n += group[2] - 1
        gath_n += sum(g[2] - 1 for g in order) + pair[2] - 1
    pad = pltpu.VMEM((frames + 2, 3, cols, chans), jnp.bfloat16)
    field = pltpu.VMEM((count, chans), jnp.float32)
    coded = pltpu.VMEM((max(land, 1), taps + 1, SUB, lanes), jnp.bfloat16)
    dma = pltpu.SemaphoreType.DMA
    vmem = pl.BlockSpec(memory_space=pltpu.VMEM)
    hbm = pl.BlockSpec(memory_space=pl.ANY)
    row = jax.ShapeDtypeStruct((1, chans), jnp.float32)
    code, *small = pl.pallas_call(
        functools.partial(kernel, sizes, plan),
        out_shape=(
            jax.ShapeDtypeStruct((parts, shares, taps + 1, SUB, lanes), jnp.bfloat16),
            row, row,
        ),
        in_specs=[hbm, hbm, vmem, vmem],
        out_specs=(hbm, vmem, vmem),
        scratch_shapes=[
            pltpu.VMEM((TAPS**3, chans, chans), jnp.bfloat16),
            pad, pad, pad,
            pltpu.VMEM((TAPS, count, chans), jnp.float32),
            field, field,
            pltpu.VMEM((count, TAPS * chans), jnp.bfloat16),
            pltpu.VMEM((count, TAPS * chans), jnp.bfloat16),
            pltpu.VMEM((parts, shares, taps, SUB, lanes), jnp.float32),
            pltpu.VMEM((parts, half, taps, SUB, lanes), jnp.float32),
            coded, coded,
            pltpu.VMEM((parts, shares, taps + 1, SUB, lanes), jnp.bfloat16),
            pltpu.VMEM(((len(rest) + 6) * SUB, chans), jnp.float32),
            pltpu.VMEM((max(small_n, 1) * SUB, chans), jnp.float32),
            dma((2,)), dma((24,)), dma((24,)), dma((TAPS,)), dma((TAPS,)),
            dma((max(parts_n, 1),)), dma((max(parts_n, 1),)),
            dma((max(gath_n, 1),)), dma((max(gath_n, 1),)),
            dma((max(small_n, 1),)), dma((max(small_n, 1),)), dma((parts,)),
        ],
        compiler_params=pltpu.CompilerParams(
            collective_id=0, has_side_effects=True, vmem_limit_bytes=60 * 1024 * 1024
        ),
    )(
        clips.reshape(frames, cols, chans),
        weight.reshape(TAPS**3, chans, chans),
        bias.reshape(1, chans),
        head.reshape(1, chans),
    )
    step = math.gcd(shares, 8)
    short = pl.BlockSpec((1, chans), lambda i: (0, 0))
    grad_weight, grad_bias, grad_head = pl.pallas_call(
        decode_kernel,
        out_shape=(jax.ShapeDtypeStruct((TAPS**3, shares, SUB, chans), jnp.float32), row, row),
        grid=(shares // step,),
        in_specs=[
            pl.BlockSpec((parts, step, taps + 1, SUB, lanes), lambda i: (0, i, 0, 0, 0)),
            short, short,
        ],
        out_specs=(
            pl.BlockSpec((TAPS**3, step, SUB, chans), lambda i: (0, i, 0, 0)), short, short
        ),
    )(code, *small)
    grad_weight = grad_weight.reshape(TAPS, TAPS, TAPS, chans, chans)
    return grad_weight, grad_bias.reshape(chans), grad_head.reshape(chans)


def solution(mesh):
    sizes = tuple(mesh.shape[axis] for axis in ("dp", "tm", "rows"))
    return jax.shard_map(
        functools.partial(per_device, sizes),
        mesh=mesh,
        in_specs=(P("dp", "tm", "rows", None, None), P(), P(), P()),
        out_specs=(P(), P(), P()),
        check_vma=False,
    )
```
